256 devices in a mesh: section: 8 (over z), dp: 32 (over x, y, core).
Axes of the slice: x: 4, y: 4, z: 8, core: 2. Of those that a mesh axis runs over, the one named last changes fastest.
Arguments:
- inject: bfloat16 [8, 256, 4096], P('section', 'dp'), may hold values from -42 to 42, as said below
- w_gate: bfloat16 [8, 4096, 11008], P('section', None, 'dp'), may hold values from -0.09375 to 0.09375
- w_up: bfloat16 [8, 4096, 11008], P('section', None, 'dp'), may hold values from -0.09375 to 0.09375
- w_down: bfloat16 [8, 11008, 4096], P('section', 'dp'), may hold values from -0.0546875 to 0.0546875
- gain: float32 [8, 4096], P('section'), may hold values from 0.5 to 1.5
Outputs:
- iterate: float32 [8, 256, 4096], P('section', 'dp')
- mixing: float32 [8, 5, 5], P('section')
The draws below stay inside these ranges and needn't reach their ends.
Inputs may be any that keep to these rules, and one draw needn't show every extreme that they name: inject has entries of varied magnitude from token to token.
All inputs are finite; a program needn't handle non-finite values.
Results may differ from the reference program's by a relative error of at most 0.0038.
Values may be sent and summed in bfloat16 or wider, within the bound.
A program may use at most 64 MiB of HBM per device.

```python
import math
import jax
import jax.numpy as jnp
from jax import lax

D = 4096
FF = 11008
ITERS = 5
HIST = 5
SECTIONS = 8
TOKENS = 256
N_DP = 32


def draw_inject(key, part):
    first = jax.random.fold_in(key, 11)
    second = jax.random.fold_in(key, 12)
    ramp = 3.0 ** (jnp.arange(TOKENS, dtype=jnp.float32) / TOKENS)
    base = jnp.clip(jax.random.normal(first, (SECTIONS, TOKENS, D), jnp.float32), -4.0, 4.0)
    scales = jnp.exp(jax.random.uniform(second, (SECTIONS, TOKENS, 1), jnp.float32, math.log(0.3), math.log(3.0)))
    values = jnp.clip(base * ramp[None, :, None] * scales, -42.0, 42.0)
    values = values.at[0, TOKENS - 1, 0].set(42.0).at[0, TOKENS - 1, 1].set(-42.0)
    return values.astype(jnp.bfloat16)


def block_levels(rng, dims, pieces, low, largest):
    def one(dim, parts):
        steps = jax.random.uniform(jax.random.fold_in(jax.random.fold_in(rng, 6), dim), (parts,), jnp.float32, low / len(pieces), largest / len(pieces))
        return jnp.repeat(jnp.exp(steps), dims[dim] // parts).reshape((-1,) + (1,) * (len(dims) - dim - 1))

    factor_of = one(*pieces[0])
    for cut in pieces[1:]:
        factor_of = factor_of * one(*cut)
    return factor_of


def bell_draw(rng, shape, spread, limit, shards=(), kind=jnp.bfloat16):
    factor_of = block_levels(rng, shape, shards, -0.22, 0.18) if shards else 1.0
    values = jax.random.normal(rng, shape, jnp.float32) * spread * factor_of
    return jnp.minimum(jnp.maximum(values, -limit), limit).astype(kind)


def setup_inputs(seed: int = 0) -> dict:
    splits = jax.random.split(jax.random.key(seed), 6)
    return {
        "inject": draw_inject(jax.random.fold_in(splits[5], 71), 0),
        "w_gate": bell_draw(splits[1], (SECTIONS, D, FF), D ** -0.5, 0.09375, ((0, 8), (2, 32))),
        "w_up": bell_draw(splits[2], (SECTIONS, D, FF), D ** -0.5, 0.09375, ((0, 8), (2, 32))),
        "w_down": bell_draw(splits[3], (SECTIONS, FF, D), FF ** -0.5, 0.0546875, ((0, 8), (1, 32))),
        "gain": jnp.clip(1.0 + 0.1 * jax.random.normal(splits[4], (SECTIONS, D), jnp.float32), 0.5, 1.5),
    }


def rms_scaled(values, gain_row):
    inverse = lax.rsqrt(lax.optimization_barrier(jnp.mean(values * values, axis=-1, keepdims=True)) + 1e-06)
    return (values * inverse * gain_row).astype(jnp.bfloat16)

def solve_small(system, target):
    count = system.shape[-1]
    entries = [[system[..., i, j] for j in range(count)] for i in range(count)]
    values = [target[..., i] for i in range(count)]
    for p in range(count):
        for i in range(p + 1, count):
            factor = entries[i][p] / entries[p][p]
            for j in range(p, count):
                entries[i][j] = entries[i][j] - factor * entries[p][j]
            values[i] = values[i] - factor * values[p]
    answer = [None] * count
    for i in range(count - 1, -1, -1):
        accum = values[i]
        for j in range(i + 1, count):
            accum = accum - entries[i][j] * answer[j]
        answer[i] = accum / entries[i][i]
    return jnp.stack(answer, axis=-1)

def mixing_weights(matrix, iteration):
    live = (jnp.arange(HIST) <= iteration).astype(jnp.float32)
    damp = 0.01 * jnp.trace(matrix, axis1=-2, axis2=-1) / (iteration + 1) + 1e-06
    eye_mat = jnp.eye(HIST, dtype=jnp.float32)
    diagonal = live * damp[..., None] + (1.0 - live)
    system = matrix * live[:, None] * live[None, :] + eye_mat * diagonal[..., None, :]
    target = jnp.broadcast_to(live, system.shape[:-1])
    beta = solve_small(system, target)
    return beta / lax.optimization_barrier(jnp.sum(beta, axis=-1, keepdims=True))

def block_out(operands):
    values, gate_w, up_w, down_w, gain_row = operands
    normed = rms_scaled(values, gain_row)
    gate_val = jnp.dot(normed, gate_w, preferred_element_type=jnp.float32)
    up_val = jnp.dot(normed, up_w, preferred_element_type=jnp.float32)
    hidden = (jax.nn.silu(gate_val) * up_val).astype(jnp.bfloat16)
    grouped = hidden.reshape(TOKENS, N_DP, FF // N_DP).transpose(1, 0, 2).astype(jnp.float32)
    down_groups = down_w.reshape(N_DP, FF // N_DP, D).astype(jnp.float32)
    partials = jnp.einsum('gtf,gfd->gtd', grouped, down_groups).astype(jnp.bfloat16).astype(jnp.float32)
    total = lax.optimization_barrier(jnp.sum(partials, axis=0))
    return (values + total).astype(jnp.bfloat16)

def reference(inject, w_gate, w_up, w_down, gain):
    source = inject.astype(jnp.float32)
    iterate = jnp.zeros((SECTIONS, TOKENS, D), jnp.float32)
    images = jnp.zeros((HIST, SECTIONS, TOKENS, D), jnp.float32)
    misfits = jnp.zeros((HIST, SECTIONS, TOKENS, D), jnp.float32)
    mixing = jnp.zeros((SECTIONS, ITERS, HIST), jnp.float32)
    cell_count = float(TOKENS * D)
    for iteration in range(ITERS):
        output = lax.map(block_out, (iterate, w_gate, w_up, w_down, gain))
        mapped = source + 0.5 * jnp.roll(output, 1, axis=0).astype(jnp.float32)
        misfit = mapped - iterate
        images = images.at[iteration].set(mapped)
        misfits = misfits.at[iteration].set(misfit)
        gram_matrix = jnp.einsum('hstd,gstd->shg', misfits, misfits, precision=lax.Precision.HIGHEST) / cell_count
        weights = mixing_weights(gram_matrix, iteration)
        mixing = mixing.at[:, iteration].set(weights)
        iterate = jnp.einsum('sh,hstd->std', weights, images, precision=lax.Precision.HIGHEST)
    return (iterate, mixing)
```

```python
import functools
import math

import jax
import jax.numpy as jnp
from jax import lax
from jax.experimental import pallas as pl
from jax.experimental.pallas import tpu as pltpu
from jax.sharding import PartitionSpec as P

ITERS = 5
HIST = 5
BF = jnp.bfloat16
F32 = jnp.float32
MESH = pl.DeviceIdType.MESH
PIECES = 4


def solve_small(entries, values):
    count = len(values)
    entries = [list(row) for row in entries]
    values = list(values)
    for p in range(count):
        for i in range(p + 1, count):
            factor = entries[i][p] / entries[p][p]
            for j in range(p, count):
                entries[i][j] = entries[i][j] - factor * entries[p][j]
            values[i] = values[i] - factor * values[p]
    answer = [None] * count
    for i in range(count - 1, -1, -1):
        accum = values[i]
        for j in range(i + 1, count):
            accum = accum - entries[i][j] * answer[j]
        answer[i] = accum / entries[i][i]
    return answer


def kernel(
    dims,
    inject_hbm, gate_hbm, up_hbm, down_hbm, gain_hbm,
    out_ref, mix_ref,
    wg_v, wu_v, wgu, wd, inj_v, gain_v,
    images, misfits, x_v, prod, rows_sq, gram, mixes,
    ybuf, meta, hid, part, r1, s2, r2, xr, xf,
    load_sem, init_send, init_recv,
    p1_send, p1_recv, p2_send, p2_recv, x_send, x_recv, h_send, h_recv,
    a1_send, a1_recv, a2_send, a2_recv, fw_send, fw_recv,
    m1_send, m1_recv, m2_send, m2_recv, mf_send, mf_recv, o_send, o_recv,
):
    n, ns, tok, feat, units, pad = dims
    rows = 2 * tok
    half = feat // 2
    width = half // PIECES
    total_rows = n * n * rows
    cells = float(total_rows * feat)
    s = lax.axis_index("section")
    d = lax.axis_index("dp")
    c = lax.rem(d, 2)
    y = lax.rem(d // 2, n)
    x = d // (2 * n)
    other = 1 - c
    below = lax.rem(s + 1, ns)
    above = lax.rem(s + ns - 1, ns)

    def at(sec, xx, yy, cc):
        return (sec, (xx * n + yy) * 2 + cc)

    def ring(i, by):
        return lax.rem(i + by, n)

    partner = at(s, x, y, other)
    along_x = [at(s, ring(x, k), y, c) for k in range(1, n)]
    along_y = [at(s, x, ring(y, k), c) for k in range(1, n)]

    def send(src, dst, ssem, rsem, dev):
        cp = pltpu.make_async_remote_copy(
            src_ref=src, dst_ref=dst, send_sem=ssem, recv_sem=rsem,
            device_id=dev, device_id_type=MESH,
        )
        cp.start()

    def wait(ref, sem):
        pltpu.make_async_copy(ref, ref, sem).wait()

    mine = pl.ds(pl.multiple_of(c * half, 128), half)
    theirs = pl.ds(pl.multiple_of(other * half, 128), half)
    own_tok = pl.ds(pl.multiple_of(c * tok, 8), tok)
    own_units = pl.ds(pl.multiple_of(c * pad, 128), units)
    loads = [
        pltpu.make_async_copy(inject_hbm.at[0, :, mine], inj_v.at[own_tok, :], load_sem.at[0]),
        pltpu.make_async_copy(gain_hbm.at[:, mine], gain_v, load_sem.at[1]),
        pltpu.make_async_copy(gate_hbm.at[0], wg_v, load_sem.at[2]),
        pltpu.make_async_copy(up_hbm.at[0], wu_v, load_sem.at[3]),
        pltpu.make_async_copy(down_hbm.at[0, :, mine], wd.at[own_units, :], load_sem.at[4]),
    ]
    for cp in loads:
        cp.start()

    barrier = pltpu.get_barrier_semaphore()
    sources = (
        [partner]
        + along_x
        + along_y
        + [at(above, xx, y, c) for xx in [ring(x, k) for k in range(n)]]
        + [at(above, x, yy, c) for yy in [ring(y, k) for k in range(1, n)]]
    )
    for dev in sources:
        pl.semaphore_signal(barrier, inc=1, device_id=dev, device_id_type=MESH)
    pl.semaphore_wait(barrier, len(sources))

    send(inject_hbm.at[0, :, theirs], inj_v.at[own_tok, :], init_send.at[0], init_recv.at[0], partner)
    send(down_hbm.at[0, :, theirs], wd.at[own_units, :], init_send.at[1], init_recv.at[1], partner)

    images[...] = jnp.zeros_like(images)
    misfits[...] = jnp.zeros_like(misfits)
    rows_sq[...] = jnp.zeros_like(rows_sq)
    gram[...] = jnp.zeros_like(gram)
    mixes[...] = jnp.zeros_like(mixes)

    lane = lax.broadcasted_iota(jnp.int32, (rows, 128), 1)
    lane8 = lax.broadcasted_iota(jnp.int32, (8, 128), 1)

    def x_first(q):
        return q % 2 == 0

    def gather_start(slot, q):
        piece = ybuf.at[slot, c, q, x, y]
        for dev in along_x if x_first(q) else along_y:
            send(piece, piece, a1_send.at[q], a1_recv.at[slot, q], dev)

    def line(slot, q):
        return ybuf.at[slot, c, q, :, y] if x_first(q) else ybuf.at[slot, c, q, x]

    def meta_start(slot):
        piece = meta.at[slot, c, x, y]
        for dev in along_x:
            send(piece, piece, m1_send, m1_recv.at[slot], dev)

    def new_image(slot, q, out_piece):
        cols = pl.ds(q * width, width)
        image = inj_v[:, cols].astype(F32) + 0.5 * out_piece
        misfit = image - x_v[:, cols]
        images[slot, :, cols] = image
        misfits[slot, :, cols] = misfit
        ybuf[slot_y(slot), c, q, x, y] = (image * gain_v[0:1, cols]).astype(BF)
        return image, misfit

    def slot_y(slot):
        return jnp.minimum(slot, ITERS - 1) if not isinstance(slot, int) else slot

    def folded(v):
        acc = v[:, 0:128]
        for g in range(1, width // 128):
            acc = acc + v[:, g * 128 : (g + 1) * 128]
        return acc

    def products(q, image, misfit, sums):
        cols = pl.ds(q * width, width)
        new = []
        for j in range(HIST):
            new.append(folded(image * images[j, :, cols]))
            new.append(folded(misfit * misfits[j, :, cols]))
        return new if sums is None else [a + b for a, b in zip(sums, new)]

    def meta_tile(slot, sums):
        tile = jnp.zeros((rows, 128), F32)
        for j in range(HIST):
            tile = tile + jnp.where(lane == j, jnp.sum(sums[2 * j], axis=1, keepdims=True), 0.0)
            tile = tile + jnp.where(lane == 8 + j, jnp.sum(sums[2 * j + 1], axis=1, keepdims=True), 0.0)
        meta[slot, c, x, y] = tile

    def meta_second(slot):
        wait(r_meta(slot), m1_recv.at[slot])
        group = meta.at[slot, c, :, y]
        for dev in along_y:
            send(group, group, m2_send, m2_recv.at[slot], dev)

    def r_meta(slot):
        return meta.at[slot, 0, 0, pl.ds(0, n - 1)]

    def meta_third(slot):
        wait(meta.at[slot, 0, pl.ds(0, n - 1)], m2_recv.at[slot])
        whole = meta.at[slot, c]
        send(whole, whole, mf_send, mf_recv.at[slot], partner)

    def meta_done(slot):
        wait(meta.at[slot, 0], mf_recv.at[slot])

    def meta_sends_done(slot):
        wait(r_meta(slot), m1_send)
        wait(meta.at[slot, 0, pl.ds(0, n - 1)], m2_send)
        wait(meta.at[slot, 0], mf_send)

    def mix(slot):
        both = (meta[slot, 0] + meta[slot, 1]).reshape(total_rows, 128)
        rows_sq[slot] = both
        sums = jnp.sum(both.reshape(total_rows // 8, 8, 128), axis=0)
        sums = jnp.broadcast_to(jnp.sum(sums, axis=0, keepdims=True), (8, 128)) / cells
        for j in range(HIST):
            entry = jnp.sum(jnp.where(lane8 == 8 + j, sums, 0.0), axis=1, keepdims=True)
            entry = jnp.broadcast_to(entry, (8, 128))
            gram[slot, j] = entry
            gram[j, slot] = entry
        live = [jnp.where(i <= slot, 1.0, 0.0).astype(F32) for i in range(HIST)]
        matrix = [[gram[i, j] for j in range(HIST)] for i in range(HIST)]
        trace = matrix[0][0]
        for i in range(1, HIST):
            trace = trace + matrix[i][i]
        damp = 0.01 * trace / jnp.full((8, 128), slot + 1, jnp.int32).astype(F32) + 1e-06
        system = [
            [
                matrix[i][j] * (live[i] * live[j])
                + ((live[i] * damp + (1.0 - live[i])) if i == j else 0.0)
                for j in range(HIST)
            ]
            for i in range(HIST)
        ]
        beta = solve_small(system, [jnp.full((8, 128), live[i], F32) for i in range(HIST)])
        norm = beta[0]
        for i in range(1, HIST):
            norm = norm + beta[i]
        weights = [b / norm for b in beta]
        row = jnp.zeros((8, 128), F32)
        for i in range(HIST):
            row = row + jnp.where(lane8 == i, weights[i], 0.0)
        mixes[slot] = row
        return weights

    def mixed_images(weights, cols):
        acc = weights[0][0:1, 0:1] * images[0, :, cols]
        for i in range(1, HIST):
            acc = acc + weights[i][0:1, 0:1] * images[i, :, cols]
        return acc

    loads[0].wait()
    loads[1].wait()
    wait(inj_v.at[own_tok, :], init_recv.at[0])
    x_v[...] = jnp.zeros_like(x_v)
    sums = None
    for q in range(PIECES):
        image, misfit = new_image(0, q, jnp.zeros((rows, width), F32))
        gather_start(0, q)
        sums = products(q, image, misfit, sums)
    meta_tile(0, sums)
    meta_start(0)

    loads[2].wait()
    loads[3].wait()
    step = 256

    def place(i, _):
        at_rows = pl.ds(pl.multiple_of(i * step, step), step)
        zeros = jnp.zeros((step, pad - units), BF)
        wgu[at_rows, 0:units] = wg_v[at_rows, :]
        wgu[at_rows, units:pad] = zeros
        wgu[at_rows, pad : pad + units] = wu_v[at_rows, :]
        wgu[at_rows, pad + units : 2 * pad] = zeros
        return 0

    lax.fori_loop(0, feat // step, place, 0)
    wd[units:pad, :] = jnp.zeros((pad - units, half), BF)
    wd[pad + units : 2 * pad, :] = jnp.zeros((pad - units, half), BF)
    prod[...] = jnp.zeros_like(prod)
    loads[4].wait()
    wait(wd.at[own_units, :], init_recv.at[1])
    wait(inj_v.at[own_tok, :], init_send.at[0])
    wait(wd.at[own_units, :], init_send.at[1])

    def matmul(slot, side, q, first):
        at_rows = pl.ds(pl.multiple_of(side * half + q * width, width), width)
        lhs = ybuf[slot, side, q].reshape(total_rows, width)
        got = jnp.dot(lhs, wgu[at_rows, :], preferred_element_type=F32)
        if first:
            prod[slot] = got
        else:
            prod[slot] += got

    def body(k, _):
        for q in range(PIECES):
            wait(ybuf.at[k, 0, 0, 0, pl.ds(0, n - 1)], a1_recv.at[k, q])
            group = line(k, q)
            for dev in along_y if x_first(q) else along_x:
                send(group, group, a2_send.at[q], a2_recv.at[k, q], dev)
        meta_second(k)
        for q in range(PIECES):
            wait(ybuf.at[k, 0, 0, pl.ds(0, n - 1)], a2_recv.at[k, q])
            whole = ybuf.at[k, c, q]
            send(whole, whole, fw_send.at[q], fw_recv.at[k, q], partner)
            if q == PIECES - 2:
                meta_third(k)
            matmul(k, c, q, q == 0)
        for q in range(PIECES - 1):
            wait(ybuf.at[k, 0, 0], fw_recv.at[k, q])
            matmul(k, other, q, False)
        for q in range(PIECES):
            wait(ybuf.at[k, 0, 0, 0, pl.ds(0, n - 1)], a1_send.at[q])
        meta_done(k)
        weights = mix(k)
        for q in range(PIECES):
            cols = pl.ds(q * width, width)
            x_v[:, cols] = mixed_images(weights, cols)
        send(x_v, xr.at[k], x_send, x_recv.at[k], at(below, x, y, c))
        acc = jnp.zeros((total_rows // 8, 8, 128), F32)
        for i in range(ITERS - 1):
            vec = jnp.zeros((8, 128), F32)
            for j in range(i + 1):
                vec = vec + jnp.where(lane8 == j, weights[j] * (1.0 if j == i else 2.0), 0.0)
            acc = acc + rows_sq[i].reshape(total_rows // 8, 8, 128) * (weights[i] * vec)[None]
        mean_sq = jnp.sum(acc.reshape(total_rows, 128), axis=1, keepdims=True) / float(feat)
        xf[...] = jnp.broadcast_to(
            lax.rsqrt(jnp.maximum(mean_sq, 0.0) + 1e-06), (total_rows, 128)
        )
        wait(ybuf.at[k, 0, 0], fw_recv.at[k, PIECES - 1])
        matmul(k, other, PIECES - 1, False)

        group_rows = 64
        own_hid = pl.ds(pl.multiple_of(c * pad, 128), pad)

        def hidden(i, _):
            at_rows = pl.ds(pl.multiple_of(i * group_rows, group_rows), group_rows)
            scale = xf[at_rows, 0:1]

            def mixed(first):
                got = weights[0][0:1, 0:1] * prod[0, at_rows, pl.ds(first, pad)]
                for j in range(1, ITERS - 1):
                    got = got + weights[j][0:1, 0:1] * prod[j, at_rows, pl.ds(first, pad)]
                return got * scale

            gate = mixed(0)
            up = mixed(pad)
            hid[at_rows, own_hid] = (gate / (1.0 + jnp.exp(-gate)) * up).astype(BF)
            return 0

        lax.fori_loop(0, total_rows // group_rows, hidden, 0)
        send(hid.at[:, own_hid], hid.at[:, own_hid], h_send, h_recv.at[k], partner)
        wait(hid.at[:, own_hid], h_recv.at[k])

        for q in range(PIECES):
            got = jnp.dot(hid[...], wd[:, q * width : (q + 1) * width], preferred_element_type=F32)
            part[q] = got.astype(BF).reshape(n, n, rows, width)
            for g in range(1, n):
                if x_first(q):
                    yy = ring(y, g)
                    src, dev = part.at[q, :, yy], at(s, x, yy, c)
                else:
                    xx = ring(x, g)
                    src, dev = part.at[q, xx], at(s, xx, y, c)
                send(src, r1.at[k, q, g - 1], p1_send.at[q], p1_recv.at[k, q], dev)
        for q in range(PIECES):
            wait(r1.at[k, q], p1_recv.at[k, q])
            own = part[q, :, y] if x_first(q) else part[q, x]
            got = own.astype(F32)
            for g in range(n - 1):
                got = got + r1[k, q, g].astype(F32)
            s2[q] = got.astype(BF)
            for g in range(n):
                if x_first(q):
                    dst, dev, place_at = ring(x, g), at(below, ring(x, g), y, c), x
                else:
                    dst, dev, place_at = ring(y, g), at(below, x, ring(y, g), c), y
                send(s2.at[q, dst], r2.at[k, q, place_at], p2_send.at[q], p2_recv.at[k, q], dev)
        wait(xr.at[k], x_recv.at[k])
        sums = None
        for q in range(PIECES):
            cols = pl.ds(q * width, width)
            wait(r2.at[k, q], p2_recv.at[k, q])
            got = r2[k, q, 0].astype(F32)
            for g in range(1, n):
                got = got + r2[k, q, g].astype(F32)
            out = (xr[k, :, cols] + got).astype(BF).astype(F32)
            image, misfit = new_image(k + 1, q, out)

            @pl.when(k < ITERS - 2)
            def _():
                gather_start(k + 1, q)

            sums = products(q, image, misfit, sums)
        meta_tile(k + 1, sums)

        for q in range(PIECES):
            wait(ybuf.at[k, 0, 0, pl.ds(0, n - 1)], a2_send.at[q])
            wait(ybuf.at[k, 0, 0], fw_send.at[q])
            wait(r1.at[k, q], p1_send.at[q])
            wait(r2.at[k, q], p2_send.at[q])
        meta_sends_done(k)
        wait(xr.at[k], x_send)
        wait(hid.at[:, own_hid], h_send)
        meta_start(k + 1)
        return 0

    def run(k, carry):
        return body(k, carry)

    lax.fori_loop(0, ITERS - 1, run, 0)

    last = ITERS - 1
    meta_second(last)
    meta_third(last)
    meta_done(last)
    weights = mix(last)
    for q in range(PIECES):
        cols = pl.ds(q * width, width)
        x_v[:, cols] = mixed_images(weights, cols)
    their_tok = pl.ds(pl.multiple_of(other * tok, 8), tok)
    send(x_v.at[their_tok, :], out_ref.at[0, :, mine], o_send, o_recv, partner)
    out_ref[0, :, mine] = x_v[own_tok, :]
    for i in range(ITERS):
        mix_ref[0, i : i + 1, :] = mixes[i, 0:1, 0:HIST]
    meta_sends_done(last)
    wait(x_v.at[their_tok, :], o_recv)
    wait(x_v.at[their_tok, :], o_send)


def local(inject, w_gate, w_up, w_down, gain):
    ns = lax.axis_size("section")
    ndp = lax.axis_size("dp")
    n = math.isqrt(ndp // 2)
    tok, feat = inject.shape[1], inject.shape[2]
    units = w_gate.shape[2]
    pad = -(-units // 128) * 128
    rows, half = 2 * tok, feat // 2
    width = half // PIECES
    total_rows = n * n * rows
    dims = (n, ns, tok, feat, units, pad)
    any_space = pl.BlockSpec(memory_space=pl.ANY)
    vmem = pl.BlockSpec(memory_space=pltpu.VMEM)
    dma = pltpu.SemaphoreType.DMA
    steps = ITERS - 1
    return pl.pallas_call(
        functools.partial(kernel, dims),
        name="fixed_point",
        out_shape=(
            jax.ShapeDtypeStruct((1, tok, feat), F32),
            jax.ShapeDtypeStruct((1, ITERS, HIST), F32),
        ),
        in_specs=[any_space] * 5,
        out_specs=(vmem, vmem),
        scratch_shapes=[
            pltpu.VMEM((feat, units), BF),
            pltpu.VMEM((feat, units), BF),
            pltpu.VMEM((feat, 2 * pad), BF),
            pltpu.VMEM((2 * pad, half), BF),
            pltpu.VMEM((rows, half), BF),
            pltpu.VMEM((1, half), F32),
            pltpu.VMEM((HIST, rows, half), F32),
            pltpu.VMEM((HIST, rows, half), F32),
            pltpu.VMEM((rows, half), F32),
            pltpu.VMEM((steps, total_rows, 2 * pad), F32),
            pltpu.VMEM((HIST, total_rows, 128), F32),
            pltpu.VMEM((HIST, HIST, 8, 128), F32),
            pltpu.VMEM((ITERS, 8, 128), F32),
            pltpu.VMEM((ITERS, 2, PIECES, n, n, rows, width), BF),
            pltpu.VMEM((ITERS, 2, n, n, rows, 128), F32),
            pltpu.VMEM((total_rows, 2 * pad), BF),
            pltpu.VMEM((PIECES, n, n, rows, width), BF),
            pltpu.VMEM((steps, PIECES, n - 1, n, rows, width), BF),
            pltpu.VMEM((PIECES, n, rows, width), BF),
            pltpu.VMEM((steps, PIECES, n, rows, width), BF),
            pltpu.VMEM((steps, rows, half), F32),
            pltpu.VMEM((total_rows, 128), F32),
            dma((5,)), dma((2,)), dma((2,)),
            dma((PIECES,)), dma((steps, PIECES)),
            dma((PIECES,)), dma((steps, PIECES)),
            dma(()), dma((steps,)),
            dma(()), dma((steps,)),
            dma((PIECES,)), dma((steps, PIECES)),
            dma((PIECES,)), dma((steps, PIECES)),
            dma((PIECES,)), dma((steps, PIECES)),
            dma(()), dma((ITERS,)),
            dma(()), dma((ITERS,)),
            dma(()), dma((ITERS,)),
            dma(()), dma(()),
        ],
        compiler_params=pltpu.CompilerParams(
            collective_id=0, has_side_effects=True, vmem_limit_bytes=63 << 20
        ),
    )(inject, w_gate, w_up, w_down, gain)


def solution(mesh):
    placed = (
        P("section", "dp", None),
        P("section", None, "dp"),
        P("section", None, "dp"),
        P("section", "dp", None),
        P("section", None),
    )
    return jax.shard_map(
        local,
        mesh=mesh,
        in_specs=placed,
        out_specs=(P("section", "dp", None), P("section", None, None)),
        check_vma=False,
    )
```
